32 devices in a mesh: dp: 8 (over z, y), tensor: 4 (over x, core).
Axes of the slice: x: 2, y: 2, z: 4, core: 2. Of those that a mesh axis runs over, the one named last changes fastest.
Arguments:
- tokens_in: bfloat16 [1024, 4096], P(('dp', 'tensor')), may hold values from -6 to 6
- grad_out: bfloat16 [1024, 4096], P(('dp', 'tensor')), may hold values from -6 to 6
- gate_pre: bfloat16 [1024, 7168], P('dp', 'tensor'), may hold values from -6 to 6
- up_pre: bfloat16 [1024, 7168], P('dp', 'tensor'), may hold values from -6 to 6
- gate_weight: bfloat16 [4096, 7168], P('dp', 'tensor'), may hold values from -0.09375 to 0.09375
- up_weight: bfloat16 [4096, 7168], P('dp', 'tensor'), may hold values from -0.09375 to 0.09375
- down_weight: bfloat16 [7168, 4096], P('tensor', 'dp'), may hold values from -0.0625 to 0.0625
- norm_gain: float32 [4096], replicated, may hold values from 0.1 to 1.9
Outputs:
- input_grad: bfloat16 [1024, 4096], P(('dp', 'tensor'))
- gain_grad: float32 [4096], replicated
- down_grad: bfloat16 [7168, 4096], P('tensor', 'dp')
The draws below stay inside these ranges and needn't reach their ends.
All inputs are finite; a program needn't handle non-finite values.
Results may differ from the reference program's by a relative error of at most 0.015.
Values may be sent and summed in bfloat16 or wider, within the bound.
A program may use at most 64 MiB of HBM per device.

```python
import jax
import jax.numpy as jnp
from jax import lax

D = 4096
FF = 7168
TOKENS = 1024
N_TENSOR = 4


def block_levels(key, extent, shards, smallest, top_value):
    factor_of, own = 1.0, jax.random.fold_in(key, 6)
    for dim, parts in shards:
        heights = jnp.exp(jax.random.uniform(jax.random.fold_in(own, dim), (parts,), jnp.float32, smallest / len(shards), top_value / len(shards)))
        factor_of = factor_of * jnp.repeat(heights, extent[dim] // parts).reshape([-1 if axis == dim else 1 for axis in range(len(extent))])
    return factor_of


def gaussian(rng, dims, deviation, most, pieces=(), kind=jnp.bfloat16):
    array = jax.random.normal(rng, dims, jnp.float32) * deviation
    if len(pieces) > 0:
        array = block_levels(rng, dims, pieces, -0.22, 0.18) * array
    return jnp.clip(array, min=-most, max=most).astype(kind)


def setup_inputs(seed: int = 0) -> dict:
    keys = jax.random.split(jax.random.key(seed), 9)
    return {
        "tokens_in": gaussian(keys[0], (TOKENS, D), 1.0, 6.0, ((0, 32),)),
        "grad_out": gaussian(keys[1], (TOKENS, D), 1.0, 6.0, ((0, 32),)),
        "gate_pre": gaussian(keys[2], (TOKENS, FF), 1.0, 6.0, ((0, 8), (1, 4))),
        "up_pre": gaussian(keys[3], (TOKENS, FF), 1.0, 6.0, ((0, 8), (1, 4))),
        "gate_weight": gaussian(keys[4], (D, FF), D ** -0.5, 0.09375, ((0, 8), (1, 4))),
        "up_weight": gaussian(keys[5], (D, FF), D ** -0.5, 0.09375, ((0, 8), (1, 4))),
        "down_weight": gaussian(keys[6], (FF, D), FF ** -0.5, 0.0625, ((0, 4), (1, 8))),
        "norm_gain": jnp.clip(1.0 + 0.18 * jax.random.normal(keys[7], (D,), jnp.float32), 0.1, 1.9),
    }


def reference(tokens_in, grad_out, gate_pre, up_pre, gate_weight, up_weight, down_weight, norm_gain):
    gate_value = gate_pre.astype(jnp.float32)
    up_value = up_pre.astype(jnp.float32)
    gate_sigmoid = jax.nn.sigmoid(gate_value)
    gate_silu = gate_value * gate_sigmoid
    act = (gate_silu * up_value).astype(jnp.bfloat16)
    grad_act = jnp.dot(grad_out, down_weight.T, preferred_element_type=jnp.float32)
    grad_gate = (grad_act * up_value * gate_sigmoid * (1.0 + gate_value * (1.0 - gate_sigmoid))).astype(jnp.bfloat16)
    grad_up = (grad_act * gate_silu).astype(jnp.bfloat16)
    down_grad = jnp.dot(act.T, grad_out, preferred_element_type=jnp.float32).astype(jnp.bfloat16)
    width = FF // N_TENSOR

    def add_shard(total, index):
        start = index * width
        gate_cols = lax.dynamic_slice_in_dim(grad_gate, start, width, 1)
        up_cols = lax.dynamic_slice_in_dim(grad_up, start, width, 1)
        gate_part = lax.dynamic_slice_in_dim(gate_weight, start, width, 1)
        up_part = lax.dynamic_slice_in_dim(up_weight, start, width, 1)
        part = jnp.dot(gate_cols, gate_part.T, preferred_element_type=jnp.float32)
        part = part + jnp.dot(up_cols, up_part.T, preferred_element_type=jnp.float32)
        return (total + lax.optimization_barrier(part.astype(jnp.bfloat16)).astype(jnp.float32), None)
    grad_norm, unused_two = lax.scan(add_shard, jnp.zeros((TOKENS, D), jnp.float32), jnp.arange(N_TENSOR, dtype=jnp.int32))
    inputs = tokens_in.astype(jnp.float32)
    inv_rms = lax.rsqrt(lax.optimization_barrier(jnp.mean(inputs * inputs, axis=1, keepdims=True)) + 1e-05)
    normed = inputs * inv_rms
    gain_grad = lax.optimization_barrier(jnp.sum(grad_norm * normed, axis=0))
    scaled = grad_norm * norm_gain
    inner = lax.optimization_barrier(jnp.mean(scaled * normed, axis=1, keepdims=True))
    input_grad = (grad_out.astype(jnp.float32) + inv_rms * (scaled - normed * inner)).astype(jnp.bfloat16)
    return (input_grad, gain_grad, down_grad)
```

```python
import functools

import jax
import jax.numpy as jnp
from jax import lax
from jax.experimental import pallas as pl
from jax.experimental.pallas import tpu as pltpu
from jax.sharding import PartitionSpec as P

MESH = pl.DeviceIdType.MESH
F32 = jnp.float32
BF16 = jnp.bfloat16
NT = (((1,), (1,)), ((), ()))
TN = (((0,), (0,)), ((), ()))


def split_line(n_dp):
    assert n_dp % 4 == 0
    return n_dp // 2


def body(
    n_dp,
    n_t,
    chunks,
    tok_ref,
    out_ref,
    gate_ref,
    up_ref,
    wg_ref,
    wu_ref,
    wd_ref,
    gain_ref,
    ig_ref,
    gg_out_ref,
    dg_ref,
    x4,
    x2,
    aall,
    ysend,
    yrecv,
    own,
    zsend,
    zin,
    gg,
    npb,
    nrv,
    gs,
    fin,
    gbuf,
    hbuf,
    s1_s,
    s1_r,
    s2_s,
    s2_r,
    ys_s,
    ys_r,
    a_s,
    a_r,
    z_s,
    z_r,
    b_s,
    b_r,
    n_s,
    n_r,
    f_s,
    f_r,
    g_s,
    g_r,
    h_s,
    h_r,
):
    r, width = tok_ref.shape
    rows, hidden = gate_ref.shape
    cols = wg_ref.shape[0]
    line = split_line(n_dp)
    rc = rows // chunks
    d = lax.axis_index("dp")
    t = lax.axis_index("tensor")
    z = d // 2
    y = d % 2
    other = 1 - y
    pair = z * 2 + other

    def loop(n, f, start=0):
        def step(i, carry):
            f(i)
            return carry

        lax.fori_loop(start, n, step, 0)

    def dp_peer(k):
        return lax.rem(d + k, n_dp)

    def t_peer(k):
        return lax.rem(t + k, n_t)

    def rcopy(src, dst, ss, rs, dd, tt):
        return pltpu.make_async_remote_copy(
            src_ref=src,
            dst_ref=dst,
            send_sem=ss,
            recv_sem=rs,
            device_id={"dp": dd, "tensor": tt},
            device_id_type=MESH,
        )

    barrier = pltpu.get_barrier_semaphore()
    loop(
        n_dp,
        lambda k: pl.semaphore_signal(
            barrier, inc=1, device_id={"dp": dp_peer(k), "tensor": t}, device_id_type=MESH
        ),
        1,
    )
    loop(
        n_t,
        lambda k: pl.semaphore_signal(
            barrier, inc=1, device_id={"dp": d, "tensor": t_peer(k)}, device_id_type=MESH
        ),
        1,
    )
    pl.semaphore_wait(barrier, n_dp + n_t - 2)

    def col(i):
        return pl.ds(pl.multiple_of(i * cols, cols), cols)

    def first(k, tgt):
        return rcopy(
            out_ref.at[:, col(tgt)], x4.at[d, t], s1_s.at[k], s1_r.at[d], tgt, t
        )

    def first_in(src):
        return rcopy(out_ref.at[:, col(0)], x4.at[src, t], s1_s.at[0], s1_r.at[src], d, t)

    loop(n_dp, lambda k: first(k, dp_peer(k)).start(), 1)

    def second(src, j):
        return rcopy(
            x4.at[src, t], x4.at[src, t], s2_s.at[src, j], s2_r.at[src, t], d, t_peer(j)
        )

    def second_in(src, tt):
        return rcopy(x4.at[src, tt], x4.at[src, tt], s2_s.at[src, 0], s2_r.at[src, tt], d, t)

    def second_own(j):
        return rcopy(
            out_ref.at[:, col(d)], x4.at[d, t], s2_s.at[d, j], s2_r.at[d, t], d, t_peer(j)
        )

    x4[d, t] = out_ref[:, col(d)]
    loop(n_t, lambda j: second_own(j).start(), 1)

    gate = gate_ref[...].astype(F32)
    aall[d] = (gate * jax.nn.sigmoid(gate) * up_ref[...].astype(F32)).astype(BF16)

    def up_copy(unit, ss, rs, src, c):
        return rcopy(unit(src * 2 + y, c), unit(src * 2 + y, c), ss.at[0, src, c], rs.at[0, src, c], d + 2, t)

    def down_copy(unit, ss, rs, src, c):
        return rcopy(unit(src * 2 + y, c), unit(src * 2 + y, c), ss.at[1, src, c], rs.at[1, src, c], d - 2, t)

    def pair_copy(unit, ss, rs, src, c):
        return rcopy(unit(src * 2 + y, c), unit(src * 2 + y, c), ss.at[2, src, c], rs.at[2, src, c], pair, t)

    def arrived(unit, ss, rs, way, src, side, c):
        u = unit(src * 2 + side, c)
        rcopy(u, u, ss.at[way, src, c], rs.at[way, src, c], d, t).wait_recv()

    def gather_own(unit, ss, rs, c):
        @pl.when(z < line - 1)
        def _():
            up_copy(unit, ss, rs, z, c).start()

        @pl.when(z > 0)
        def _():
            down_copy(unit, ss, rs, z, c).start()

        pair_copy(unit, ss, rs, z, c).start()

    def gather_step(unit, ss, rs, s, n_c):
        for c in range(n_c):
            low, high = z - s, z + s

            @pl.when(low >= 0)
            def _():
                arrived(unit, ss, rs, 0, low, y, c)

                @pl.when(z < line - 1)
                def _():
                    up_copy(unit, ss, rs, low, c).start()

                pair_copy(unit, ss, rs, low, c).start()

            @pl.when(high < line)
            def _():
                arrived(unit, ss, rs, 1, high, y, c)

                @pl.when(z > 0)
                def _():
                    down_copy(unit, ss, rs, high, c).start()

                pair_copy(unit, ss, rs, high, c).start()

    def gather_drain(unit, ss, rs, n_c):
        def one(src):
            for c in range(n_c):

                @pl.when((src <= z) & (z < line - 1))
                def _():
                    up_copy(unit, ss, rs, src, c).wait_send()

                @pl.when((src >= z) & (z > 0))
                def _():
                    down_copy(unit, ss, rs, src, c).wait_send()

                pair_copy(unit, ss, rs, src, c).wait_send()

        loop(line, one)

    def act_unit(i, c):
        return aall.at[i]

    gather_own(act_unit, a_s, a_r, 0)

    def relay(k):
        src = lax.rem(d + n_dp - k, n_dp)
        first_in(src).wait_recv()
        loop(n_t, lambda j: second(src, j).start(), 1)

    loop(n_dp, relay, 1)

    def settle(src):
        loop(n_t, lambda j: second_in(src, t_peer(j)).wait_recv(), 1)
        x2[src] = x4[src].astype(F32).reshape(rows, cols).astype(BF16)

    loop(n_dp, settle)

    def cs(c):
        return pl.ds(c * rc, rc)

    def pair_part(zz, c):
        return rcopy(
            ysend.at[zz, cs(c)], yrecv.at[zz, cs(c)], ys_s.at[zz, c], ys_r.at[zz, c], pair, t
        )

    def partial(i):
        return lax.dot_general(x2[i], wd_ref[...], NT, preferred_element_type=F32)

    def send_parts(p):
        def make(q):
            zz = jnp.where(q == 0, line - 1 - p, p)
            ysend[zz] = partial(zz * 2 + other).astype(BF16)

        loop(2, make)
        for c in range(chunks):
            pair_part(line - 1 - p, c).start()
            pair_part(p, c).start()

    loop(line // 2, send_parts)

    def keep(zz):
        own[zz] = partial(zz * 2 + y)

    loop(line, keep)

    loop(line, lambda s: gather_step(act_unit, a_s, a_r, s, 1), 1)

    def line_part(way, zz, c):
        return rcopy(
            zsend.at[zz, cs(c)],
            zin.at[way, zz, cs(c)],
            z_s.at[zz, c],
            z_r.at[way, zz, c],
            d + 2 - 4 * way,
            t,
        )

    def line_in(way, zz, c):
        rcopy(
            zsend.at[zz, cs(c)], zin.at[way, zz, cs(c)], z_s.at[zz, c], z_r.at[way, zz, c], d, t
        ).wait_recv()

    def reduce_one(zz, c):
        pair_part(zz, c).wait_recv()
        own[zz, cs(c)] += yrecv[zz, cs(c)].astype(F32)

        def send_on(way, has_before):
            @pl.when(has_before)
            def _():
                line_in(way, zz, c)
                own[zz, cs(c)] += zin[way, zz, cs(c)].astype(F32)

            zsend[zz, cs(c)] = own[zz, cs(c)].astype(BF16)
            line_part(way, zz, c).start()

        @pl.when(zz > z)
        def _():
            send_on(0, z > 0)

        @pl.when(zz < z)
        def _():
            send_on(1, z < line - 1)

    def reduce_pairs(p):
        for c in range(chunks):
            reduce_one(line - 1 - p, c)
            reduce_one(p, c)

    loop(line // 2, reduce_pairs)

    def grad_unit(i, c):
        return gg.at[i, :, cs(c)]

    for c in range(chunks):

        @pl.when(z > 0)
        def _():
            line_in(0, z, c)
            own[z, cs(c)] += zin[0, z, cs(c)].astype(F32)

        @pl.when(z < line - 1)
        def _():
            line_in(1, z, c)
            own[z, cs(c)] += zin[1, z, cs(c)].astype(F32)

        grad_act = own[z, cs(c)]
        gate = gate_ref[cs(c), :].astype(F32)
        sig = jax.nn.sigmoid(gate)
        gg[d, 0, cs(c)] = (
            grad_act * up_ref[cs(c), :].astype(F32) * sig * (1.0 + gate * (1.0 - sig))
        ).astype(BF16)
        gg[d, 1, cs(c)] = (grad_act * (gate * sig)).astype(BF16)
        gather_own(grad_unit, b_s, b_r, c)

    loop(line, lambda src: arrived(act_unit, a_s, a_r, 2, src, other, 0))
    tile = 256 if hidden % 256 == 0 else hidden

    def down_tile(i):
        if tile == hidden:
            sl = slice(None)
        else:
            sl = pl.ds(pl.multiple_of(i * tile, tile), tile)
        left = aall[:, :, sl].reshape(n_dp * rows, tile)
        right = x2[...].reshape(n_dp * rows, cols)
        res = lax.dot_general(left, right, TN, preferred_element_type=F32).astype(BF16)
        if tile == hidden:
            dg_ref[...] = res
        else:
            dg_ref[sl, :] = res

    loop(hidden // tile, down_tile)

    def norm_copy(i, j):
        tt = t_peer(j)
        return rcopy(npb.at[i, tt], nrv.at[i, t], n_s.at[i, j], n_r.at[i, t], d, tt)

    def norm_block(i):
        part = lax.dot_general(gg[i, 0], wg_ref[...], NT, preferred_element_type=F32)
        part = part + lax.dot_general(gg[i, 1], wu_ref[...], NT, preferred_element_type=F32)
        npb[i] = part.reshape(n_t, r, cols).astype(BF16)
        loop(n_t, lambda j: norm_copy(i, j).start(), 1)

    def visit(s):
        @pl.when((s > 0) & (s < line))
        def _():
            gather_step(grad_unit, b_s, b_r, s, chunks)

        def one(q):
            dist = s - q // 2
            src = jnp.where(q % 2 == 0, z - dist, z + dist)
            ok = (dist >= 0) & (src >= 0) & (src < line) & ((dist > 0) | (q % 2 == 0))

            @pl.when(ok)
            def _():
                @pl.when(q >= 2)
                def _():
                    for c in range(chunks):
                        arrived(grad_unit, b_s, b_r, 2, src, other, c)

                norm_block(src * 2 + jnp.where(q >= 2, other, y))

        loop(4, one)

    loop(line + 1, visit)

    def fin_copy(i):
        return rcopy(gs.at[i], fin.at[d], f_s.at[i], f_r.at[d], i, t)

    def combine(k):
        i = dp_peer(k)

        def add(j, acc):
            tt = t_peer(j)
            rcopy(npb.at[i, tt], nrv.at[i, tt], n_s.at[i, 0], n_r.at[i, tt], d, t).wait_recv()
            return acc + nrv[i, tt].astype(F32)

        acc = lax.fori_loop(1, n_t, add, npb[i, t].astype(F32)).astype(BF16)

        @pl.when(k > 0)
        def _():
            gs[i] = acc
            fin_copy(i).start()

        @pl.when(k == 0)
        def _():
            fin[d] = acc

    loop(n_dp, combine)

    total = jnp.zeros((r, 1), F32)
    for i in range(n_dp):
        v = tok_ref[:, i * cols : (i + 1) * cols].astype(F32)
        total = total + jnp.sum(v * v, axis=1, keepdims=True)
    inv = lax.rsqrt(total / width + 1e-05)

    def fin_in(k):
        i = dp_peer(k)
        rcopy(gs.at[i], fin.at[i], f_s.at[i], f_r.at[i], d, t).wait_recv()

    loop(n_dp, fin_in, 1)

    inner = jnp.zeros((r, 1), F32)
    for i in range(n_dp):
        sl = slice(i * cols, (i + 1) * cols)
        prod = fin[i].astype(F32) * (tok_ref[:, sl].astype(F32) * inv)
        gbuf[t, :, sl] = jnp.sum(prod, axis=0, keepdims=True)
        inner = inner + jnp.sum(prod * gain_ref[:, sl], axis=1, keepdims=True)
    inner = inner / width

    def gain_copy(j):
        return rcopy(gbuf.at[t], gbuf.at[t], g_s.at[j], g_r.at[t], d, t_peer(j))

    loop(n_t, lambda j: gain_copy(j).start(), 1)
    for i in range(n_dp):
        sl = slice(i * cols, (i + 1) * cols)
        scaled = fin[i].astype(F32) * gain_ref[:, sl]
        normed = tok_ref[:, sl].astype(F32) * inv
        ig_ref[:, sl] = (
            out_ref[:, sl].astype(F32) + inv * (scaled - normed * inner)
        ).astype(BF16)

    def gain_in(j):
        tt = t_peer(j)
        rcopy(gbuf.at[tt], gbuf.at[tt], g_s.at[0], g_r.at[tt], d, t).wait_recv()

    loop(n_t, gain_in, 1)
    hbuf[d] = jnp.sum(gbuf[...], axis=0)

    def all_copy(k):
        return rcopy(hbuf.at[d], hbuf.at[d], h_s.at[k], h_r.at[d], dp_peer(k), t)

    loop(n_dp, lambda k: all_copy(k).start(), 1)

    def all_in(k):
        i = dp_peer(k)
        rcopy(hbuf.at[i], hbuf.at[i], h_s.at[0], h_r.at[i], d, t).wait_recv()

    loop(n_dp, all_in, 1)
    gg_out_ref[...] = jnp.sum(hbuf[...], axis=0)

    loop(n_dp, lambda k: first(k, dp_peer(k)).wait_send(), 1)
    loop(n_dp, lambda i: loop(n_t, lambda j: second(i, j).wait_send(), 1))
    gather_drain(act_unit, a_s, a_r, 1)
    gather_drain(grad_unit, b_s, b_r, chunks)

    def drain_parts(zz):
        for c in range(chunks):
            pair_part(zz, c).wait_send()

            @pl.when(zz != z)
            def _():
                line_part(0, zz, c).wait_send()

    loop(line, drain_parts)
    loop(n_dp, lambda i: loop(n_t, lambda j: norm_copy(i, j).wait_send(), 1))
    loop(n_dp, lambda k: fin_copy(dp_peer(k)).wait_send(), 1)
    loop(n_t, lambda j: gain_copy(j).wait_send(), 1)
    loop(n_dp, lambda k: all_copy(k).wait_send(), 1)


def per_device(
    n_dp, n_t, tokens_in, grad_out, gate_pre, up_pre, gate_weight, up_weight, down_weight, norm_gain
):
    r, width = tokens_in.shape
    rows, hidden = gate_pre.shape
    cols = gate_weight.shape[0]
    line = split_line(n_dp)
    chunks = 4 if rows % 64 == 0 else 1
    dma = pltpu.SemaphoreType.DMA
    vmem = pl.BlockSpec(memory_space=pltpu.VMEM)
    input_grad, gain_grad, down_grad = pl.pallas_call(
        functools.partial(body, n_dp, n_t, chunks),
        out_shape=(
            jax.ShapeDtypeStruct((r, width), BF16),
            jax.ShapeDtypeStruct((1, width), F32),
            jax.ShapeDtypeStruct((hidden, cols), BF16),
        ),
        in_specs=[vmem] * 8,
        out_specs=(vmem, vmem, vmem),
        scratch_shapes=[
            pltpu.VMEM((n_dp, n_t, r, cols), BF16),
            pltpu.VMEM((n_dp, rows, cols), BF16),
            pltpu.VMEM((n_dp, rows, hidden), BF16),
            pltpu.VMEM((line, rows, hidden), BF16),
            pltpu.VMEM((line, rows, hidden), BF16),
            pltpu.VMEM((line, rows, hidden), F32),
            pltpu.VMEM((line, rows, hidden), BF16),
            pltpu.VMEM((2, line, rows, hidden), BF16),
            pltpu.VMEM((n_dp, 2, rows, hidden), BF16),
            pltpu.VMEM((n_dp, n_t, r, cols), BF16),
            pltpu.VMEM((n_dp, n_t, r, cols), BF16),
            pltpu.VMEM((n_dp, r, cols), BF16),
            pltpu.VMEM((n_dp, r, cols), BF16),
            pltpu.VMEM((n_t, 1, width), F32),
            pltpu.VMEM((n_dp, 1, width), F32),
            dma((n_dp,)),
            dma((n_dp,)),
            dma((n_dp, n_t)),
            dma((n_dp, n_t)),
            dma((line, chunks)),
            dma((line, chunks)),
            dma((3, line, 1)),
            dma((3, line, 1)),
            dma((line, chunks)),
            dma((2, line, chunks)),
            dma((3, line, chunks)),
            dma((3, line, chunks)),
            dma((n_dp, n_t)),
            dma((n_dp, n_t)),
            dma((n_dp,)),
            dma((n_dp,)),
            dma((n_t,)),
            dma((n_t,)),
            dma((n_dp,)),
            dma((n_dp,)),
        ],
        compiler_params=pltpu.CompilerParams(
            collective_id=0, has_side_effects=True, vmem_limit_bytes=63 * 2**20
        ),
    )(
        tokens_in,
        grad_out,
        gate_pre,
        up_pre,
        gate_weight,
        up_weight,
        down_weight,
        norm_gain.reshape(1, width),
    )
    return (input_grad, gain_grad.reshape(width), down_grad)


def solution(mesh):
    return jax.shard_map(
        functools.partial(per_device, mesh.shape["dp"], mesh.shape["tensor"]),
        mesh=mesh,
        in_specs=(
            P(("dp", "tensor"), None),
            P(("dp", "tensor"), None),
            P("dp", "tensor"),
            P("dp", "tensor"),
            P("dp", "tensor"),
            P("dp", "tensor"),
            P("tensor", "dp"),
            P(),
        ),
        out_specs=(P(("dp", "tensor"), None), P(), P("tensor", "dp")),
        check_vma=False,
    )
```

```python
import functools

import jax
import jax.numpy as jnp
from jax import lax
from jax.experimental import pallas as pl
from jax.experimental.pallas import tpu as pltpu
from jax.sharding import PartitionSpec as P

MESH = pl.DeviceIdType.MESH
W_CHUNKS = 4
F32 = jnp.float32
BF16 = jnp.bfloat16
NT = (((1,), (1,)), ((), ()))
TN = (((0,), (0,)), ((), ()))


def split_line(n_dp):
    assert n_dp % 4 == 0
    return n_dp // 2


def body(
    n_dp,
    n_t,
    chunks,
    tok_ref,
    out_ref,
    gate_ref,
    up_ref,
    wg_ref,
    wu_ref,
    wd_ref,
    gain_ref,
    ig_ref,
    gg_out_ref,
    dg_ref,
    x4,
    x2,
    aall,
    ysend,
    yrecv,
    own,
    zsend,
    zin,
    gg,
    wrecv,
    npb,
    nrv,
    gs,
    fin,
    gbuf,
    hbuf,
    s1_s,
    s1_r,
    s2_s,
    s2_r,
    ys_s,
    ys_r,
    a_s,
    a_r,
    z_s,
    z_r,
    b_s,
    b_r,
    w_s,
    w_r,
    n_s,
    n_r,
    f_s,
    f_r,
    g_s,
    g_r,
    h_s,
    h_r,
):
    r, width = tok_ref.shape
    rows, hidden = gate_ref.shape
    cols = wg_ref.shape[0]
    line = split_line(n_dp)
    rc = rows // chunks
    d = lax.axis_index("dp")
    t = lax.axis_index("tensor")
    z = d // 2
    y = d % 2
    other = 1 - y
    pair = z * 2 + other

    def loop(n, f, start=0):
        def step(i, carry):
            f(i)
            return carry

        lax.fori_loop(start, n, step, 0)

    def dp_peer(k):
        return lax.rem(d + k, n_dp)

    def t_peer(k):
        return lax.rem(t + k, n_t)

    def rcopy(src, dst, ss, rs, dd, tt):
        return pltpu.make_async_remote_copy(
            src_ref=src,
            dst_ref=dst,
            send_sem=ss,
            recv_sem=rs,
            device_id={"dp": dd, "tensor": tt},
            device_id_type=MESH,
        )

    barrier = pltpu.get_barrier_semaphore()
    loop(
        n_dp,
        lambda k: pl.semaphore_signal(
            barrier, inc=1, device_id={"dp": dp_peer(k), "tensor": t}, device_id_type=MESH
        ),
        1,
    )
    loop(
        n_t,
        lambda k: pl.semaphore_signal(
            barrier, inc=1, device_id={"dp": d, "tensor": t_peer(k)}, device_id_type=MESH
        ),
        1,
    )
    pl.semaphore_wait(barrier, n_dp + n_t - 2)

    def col(i):
        return pl.ds(pl.multiple_of(i * cols, cols), cols)

    def first(k, tgt):
        return rcopy(
            out_ref.at[:, col(tgt)], x4.at[d, t], s1_s.at[k], s1_r.at[d], tgt, t
        )

    def first_in(src):
        return rcopy(out_ref.at[:, col(0)], x4.at[src, t], s1_s.at[0], s1_r.at[src], d, t)

    loop(n_dp, lambda k: first(k, dp_peer(k)).start(), 1)

    def second(src, j):
        return rcopy(
            x4.at[src, t], x4.at[src, t], s2_s.at[src, j], s2_r.at[src, t], d, t_peer(j)
        )

    def second_in(src, tt):
        return rcopy(x4.at[src, tt], x4.at[src, tt], s2_s.at[src, 0], s2_r.at[src, tt], d, t)

    def second_own(j):
        return rcopy(
            out_ref.at[:, col(d)], x4.at[d, t], s2_s.at[d, j], s2_r.at[d, t], d, t_peer(j)
        )

    x4[d, t] = out_ref[:, col(d)]
    loop(n_t, lambda j: second_own(j).start(), 1)

    gate = gate_ref[...].astype(F32)
    aall[d] = (gate * jax.nn.sigmoid(gate) * up_ref[...].astype(F32)).astype(BF16)

    w_rows = cols // W_CHUNKS

    def weight_copy(n):
        a, c = n % 2, n // 2
        src = (wg_ref, wu_ref)[a].at[pl.ds(c * w_rows, w_rows)]
        return rcopy(
            src, wrecv.at[a, pl.ds(c * w_rows, w_rows)], w_s.at[a, c], w_r.at[a, c], pair, t
        )

    def up_copy(unit, ss, rs, way, src, side, c):
        u = unit(src, side, c)
        return rcopy(u, u, ss.at[way, src, c], rs.at[way, src, c], d + 2, t)

    def down_copy(unit, ss, rs, way, src, side, c):
        u = unit(src, side, c)
        return rcopy(u, u, ss.at[way + 1, src, c], rs.at[way + 1, src, c], d - 2, t)

    def arrived(unit, ss, rs, way, src, side, c):
        u = unit(src, side, c)
        rcopy(u, u, ss.at[way, src, c], rs.at[way, src, c], d, t).wait_recv()

    def gather_own(unit, ss, rs, way, side, c):
        @pl.when(z < line - 1)
        def _():
            up_copy(unit, ss, rs, way, z, side, c).start()

        @pl.when(z > 0)
        def _():
            down_copy(unit, ss, rs, way, z, side, c).start()

    def gather_step(unit, ss, rs, way, side, s, c, then=None):
        low, high = z - s, z + s

        @pl.when(low >= 0)
        def _():
            arrived(unit, ss, rs, way, low, side, c)

            @pl.when(z < line - 1)
            def _():
                up_copy(unit, ss, rs, way, low, side, c).start()

            if then is not None:
                then(low)

        @pl.when(high < line)
        def _():
            arrived(unit, ss, rs, way + 1, high, side, c)

            @pl.when(z > 0)
            def _():
                down_copy(unit, ss, rs, way, high, side, c).start()

            if then is not None:
                then(high)

    def gather_drain(unit, ss, rs, way, side, c):
        def one(src):
            @pl.when((src <= z) & (z < line - 1))
            def _():
                up_copy(unit, ss, rs, way, src, side, c).wait_send()

            @pl.when((src >= z) & (z > 0))
            def _():
                down_copy(unit, ss, rs, way, src, side, c).wait_send()

        loop(line, one)

    half = rows // 2

    def act_unit(src, side, c):
        return aall.at[src * 2 + side, pl.ds(c * half, half)]

    def act_pair(src, c):
        u = act_unit(src, y, c)
        return rcopy(u, u, a_s.at[2, src, c], a_r.at[2, src, c], pair, t)

    act_pair(z, 1).start()
    gather_own(act_unit, a_s, a_r, 0, y, 0)
    gather_own(act_unit, a_s, a_r, 0, y, 1)
    act_pair(z, 0).start()
    for n in range(2):
        weight_copy(n).start()

    def relay(k):
        src = lax.rem(d + n_dp - k, n_dp)
        first_in(src).wait_recv()
        loop(n_t, lambda j: second(src, j).start(), 1)

    loop(n_dp, relay, 1)
    arrived(act_unit, a_s, a_r, 2, z, other, 1)
    gather_own(act_unit, a_s, a_r, 3, other, 1)

    def settle(src):
        loop(n_t, lambda j: second_in(src, t_peer(j)).wait_recv(), 1)
        x2[src] = x4[src].astype(F32).reshape(rows, cols).astype(BF16)

    loop(n_dp, settle)

    def cs(c):
        return pl.ds(c * rc, rc)

    def pair_part(zz, c):
        return rcopy(
            ysend.at[zz, cs(c)], yrecv.at[zz, cs(c)], ys_s.at[zz, c], ys_r.at[zz, c], pair, t
        )

    def partial(i):
        return lax.dot_general(x2[i], wd_ref[...], NT, preferred_element_type=F32)

    def send_parts(p):
        def make(q):
            zz = jnp.where(q == 0, line - 1 - p, p)
            ysend[zz] = partial(zz * 2 + other).astype(BF16)

        loop(2, make)
        for c in range(chunks):
            pair_part(line - 1 - p, c).start()
            pair_part(p, c).start()

    loop(line // 2, send_parts)

    def keep(zz):
        own[zz] = partial(zz * 2 + y)

    loop(line, keep)

    weight_copy(2).start()

    def act_step(s):
        gather_step(
            act_unit, a_s, a_r, 0, y, s, 0, lambda src: act_pair(src, 0).start()
        )
        gather_step(act_unit, a_s, a_r, 0, y, s, 1)
        gather_step(act_unit, a_s, a_r, 3, other, s, 1)

    loop(line, act_step, 1)
    for n in range(3, 2 * W_CHUNKS):
        weight_copy(n).start()

    def line_part(way, zz, c):
        return rcopy(
            zsend.at[zz, cs(c)],
            zin.at[way, zz, cs(c)],
            z_s.at[zz, c],
            z_r.at[way, zz, c],
            d + 2 - 4 * way,
            t,
        )

    def line_in(way, zz, c):
        rcopy(
            zsend.at[zz, cs(c)], zin.at[way, zz, cs(c)], z_s.at[zz, c], z_r.at[way, zz, c], d, t
        ).wait_recv()

    def reduce_one(zz, c):
        pair_part(zz, c).wait_recv()
        own[zz, cs(c)] += yrecv[zz, cs(c)].astype(F32)

        def send_on(way, has_before):
            @pl.when(has_before)
            def _():
                line_in(way, zz, c)
                own[zz, cs(c)] += zin[way, zz, cs(c)].astype(F32)

            zsend[zz, cs(c)] = own[zz, cs(c)].astype(BF16)
            line_part(way, zz, c).start()

        @pl.when(zz > z)
        def _():
            send_on(0, z > 0)

        @pl.when(zz < z)
        def _():
            send_on(1, z < line - 1)

    def reduce_pairs(p):
        for c in range(chunks):
            reduce_one(line - 1 - p, c)
            reduce_one(p, c)

    loop(line // 2, reduce_pairs)

    def grad_unit(src, side, c):
        return gg.at[src, :, cs(c)]

    for c in range(chunks):

        @pl.when(z > 0)
        def _():
            line_in(0, z, c)
            own[z, cs(c)] += zin[0, z, cs(c)].astype(F32)

        @pl.when(z < line - 1)
        def _():
            line_in(1, z, c)
            own[z, cs(c)] += zin[1, z, cs(c)].astype(F32)

        grad_act = own[z, cs(c)]
        gate = gate_ref[cs(c), :].astype(F32)
        sig = jax.nn.sigmoid(gate)
        gg[z, 0, cs(c)] = (
            grad_act * up_ref[cs(c), :].astype(F32) * sig * (1.0 + gate * (1.0 - sig))
        ).astype(BF16)
        gg[z, 1, cs(c)] = (grad_act * (gate * sig)).astype(BF16)
        gather_own(grad_unit, b_s, b_r, 0, y, c)

    loop(line, lambda src: arrived(act_unit, a_s, a_r, 2, src, other, 0))
    tile = 256 if hidden % 256 == 0 else hidden

    def down_tile(i):
        if tile == hidden:
            sl = slice(None)
        else:
            sl = pl.ds(pl.multiple_of(i * tile, tile), tile)
        left = aall[:, :, sl].reshape(n_dp * rows, tile)
        right = x2[...].reshape(n_dp * rows, cols)
        res = lax.dot_general(left, right, TN, preferred_element_type=F32).astype(BF16)
        if tile == hidden:
            dg_ref[...] = res
        else:
            dg_ref[sl, :] = res

    loop(hidden // tile, down_tile)

    def norm_copy(side, i, j):
        tt = t_peer(j)
        return rcopy(
            npb.at[side, i, tt], nrv.at[side, i, t], n_s.at[side, i, j], n_r.at[side, i, t], d, tt
        )

    def norm_own(i):
        part = lax.dot_general(gg[i, 0], wg_ref[...], NT, preferred_element_type=F32)
        part = part + lax.dot_general(gg[i, 1], wu_ref[...], NT, preferred_element_type=F32)
        npb[y, i] = part.reshape(n_t, r, cols).astype(BF16)
        loop(n_t, lambda j: norm_copy(y, i, j).start(), 1)

    def norm_other(p):
        two = pl.ds(2 * p, 2)
        part = lax.dot_general(
            gg[two, 0].reshape(2 * rows, hidden), wrecv[0], NT, preferred_element_type=F32
        )
        part = part + lax.dot_general(
            gg[two, 1].reshape(2 * rows, hidden), wrecv[1], NT, preferred_element_type=F32
        )
        npb[other, two] = part.reshape(2, n_t, r, cols).astype(BF16)
        loop(2, lambda q: loop(n_t, lambda j: norm_copy(other, 2 * p + q, j).start(), 1))

    def fin_copy(side, i):
        return rcopy(
            gs.at[side, i], fin.at[z, side], f_s.at[side, i], f_r.at[side, z], i * 2 + y, t
        )

    def combine(side, i):
        def add(j, acc):
            tt = t_peer(j)
            rcopy(
                npb.at[side, i, tt], nrv.at[side, i, tt], n_s.at[side, i, 0], n_r.at[side, i, tt], d, t
            ).wait_recv()
            return acc + nrv[side, i, tt].astype(F32)

        acc = lax.fori_loop(1, n_t, add, npb[side, i, t].astype(F32)).astype(BF16)

        @pl.when(i != z)
        def _():
            gs[side, i] = acc
            fin_copy(side, i).start()

        @pl.when(i == z)
        def _():
            fin[z, side] = acc

    def at_distance(dist, f):
        def one(q):
            src = jnp.where(q == 0, z - dist, z + dist)

            @pl.when((src >= 0) & (src < line) & ((dist > 0) | (q == 0)))
            def _():
                f(src)

        loop(2, one)

    def visit(s):
        @pl.when(s > 0)
        def _():
            for c in range(chunks):
                gather_step(grad_unit, b_s, b_r, 0, y, s, c)

        at_distance(s, norm_own)

        @pl.when(s > 0)
        def _():
            at_distance(s - 1, lambda src: combine(y, src))

    loop(line, visit)
    for n in range(2 * W_CHUNKS):
        weight_copy(n).wait_recv()
    loop(line // 2, norm_other)
    at_distance(line - 1, lambda src: combine(y, src))
    loop(line, lambda i: combine(other, i))

    total = jnp.zeros((r, 1), F32)
    for i in range(n_dp):
        v = tok_ref[:, i * cols : (i + 1) * cols].astype(F32)
        total = total + jnp.sum(v * v, axis=1, keepdims=True)
    inv = lax.rsqrt(total / width + 1e-05)

    def fin_in(k):
        i = lax.rem(z + k, line)

        def one(side):
            rcopy(
                gs.at[side, i], fin.at[i, side], f_s.at[side, i], f_r.at[side, i], d, t
            ).wait_recv()

        loop(2, one)

    loop(line, fin_in, 1)

    inner = jnp.zeros((r, 1), F32)
    for i in range(n_dp):
        sl = slice(i * cols, (i + 1) * cols)
        prod = fin[i // 2, i % 2].astype(F32) * (tok_ref[:, sl].astype(F32) * inv)
        gbuf[t, :, sl] = jnp.sum(prod, axis=0, keepdims=True)
        inner = inner + jnp.sum(prod * gain_ref[:, sl], axis=1, keepdims=True)
    inner = inner / width

    def gain_copy(j):
        return rcopy(gbuf.at[t], gbuf.at[t], g_s.at[j], g_r.at[t], d, t_peer(j))

    loop(n_t, lambda j: gain_copy(j).start(), 1)
    for i in range(n_dp):
        sl = slice(i * cols, (i + 1) * cols)
        scaled = fin[i // 2, i % 2].astype(F32) * gain_ref[:, sl]
        normed = tok_ref[:, sl].astype(F32) * inv
        ig_ref[:, sl] = (
            out_ref[:, sl].astype(F32) + inv * (scaled - normed * inner)
        ).astype(BF16)

    def gain_in(j):
        tt = t_peer(j)
        rcopy(gbuf.at[tt], gbuf.at[tt], g_s.at[0], g_r.at[tt], d, t).wait_recv()

    loop(n_t, gain_in, 1)
    hbuf[d] = jnp.sum(gbuf[...], axis=0)

    def all_copy(k):
        return rcopy(hbuf.at[d], hbuf.at[d], h_s.at[k], h_r.at[d], dp_peer(k), t)

    loop(n_dp, lambda k: all_copy(k).start(), 1)

    def all_in(k):
        i = dp_peer(k)
        rcopy(hbuf.at[i], hbuf.at[i], h_s.at[0], h_r.at[i], d, t).wait_recv()

    loop(n_dp, all_in, 1)
    gg_out_ref[...] = jnp.sum(hbuf[...], axis=0)

    loop(n_dp, lambda k: first(k, dp_peer(k)).wait_send(), 1)
    loop(n_dp, lambda i: loop(n_t, lambda j: second(i, j).wait_send(), 1))
    for c in range(2):
        gather_drain(act_unit, a_s, a_r, 0, y, c)
    gather_drain(act_unit, a_s, a_r, 3, other, 1)
    loop(line, lambda src: act_pair(src, 0).wait_send())
    act_pair(z, 1).wait_send()
    for n in range(2 * W_CHUNKS):
        weight_copy(n).wait_send()
    for c in range(chunks):
        gather_drain(grad_unit, b_s, b_r, 0, y, c)

    def drain_parts(zz):
        for c in range(chunks):
            pair_part(zz, c).wait_send()

            @pl.when(zz != z)
            def _():
                line_part(0, zz, c).wait_send()

    loop(line, drain_parts)

    def drain_norm(side):
        loop(line, lambda i: loop(n_t, lambda j: norm_copy(side, i, j).wait_send(), 1))
        loop(line, lambda k: fin_copy(side, lax.rem(z + k, line)).wait_send(), 1)

    loop(2, drain_norm)
    loop(n_t, lambda j: gain_copy(j).wait_send(), 1)
    loop(n_dp, lambda k: all_copy(k).wait_send(), 1)


def per_device(
    n_dp, n_t, tokens_in, grad_out, gate_pre, up_pre, gate_weight, up_weight, down_weight, norm_gain
):
    r, width = tokens_in.shape
    rows, hidden = gate_pre.shape
    cols = gate_weight.shape[0]
    line = split_line(n_dp)
    chunks = 4 if rows % 64 == 0 else 1
    dma = pltpu.SemaphoreType.DMA
    vmem = pl.BlockSpec(memory_space=pltpu.VMEM)
    input_grad, gain_grad, down_grad = pl.pallas_call(
        functools.partial(body, n_dp, n_t, chunks),
        out_shape=(
            jax.ShapeDtypeStruct((r, width), BF16),
            jax.ShapeDtypeStruct((1, width), F32),
            jax.ShapeDtypeStruct((hidden, cols), BF16),
        ),
        in_specs=[vmem] * 8,
        out_specs=(vmem, vmem, vmem),
        scratch_shapes=[
            pltpu.VMEM((n_dp, n_t, r, cols), BF16),
            pltpu.VMEM((n_dp, rows, cols), BF16),
            pltpu.VMEM((n_dp, rows, hidden), BF16),
            pltpu.VMEM((line, rows, hidden), BF16),
            pltpu.VMEM((line, rows, hidden), BF16),
            pltpu.VMEM((line, rows, hidden), F32),
            pltpu.VMEM((line, rows, hidden), BF16),
            pltpu.VMEM((2, line, rows, hidden), BF16),
            pltpu.VMEM((line, 2, rows, hidden), BF16),
            pltpu.VMEM((2, cols, hidden), BF16),
            pltpu.VMEM((2, line, n_t, r, cols), BF16),
            pltpu.VMEM((2, line, n_t, r, cols), BF16),
            pltpu.VMEM((2, line, r, cols), BF16),
            pltpu.VMEM((line, 2, r, cols), BF16),
            pltpu.VMEM((n_t, 1, width), F32),
            pltpu.VMEM((n_dp, 1, width), F32),
            dma((n_dp,)),
            dma((n_dp,)),
            dma((n_dp, n_t)),
            dma((n_dp, n_t)),
            dma((line, chunks)),
            dma((line, chunks)),
            dma((5, line, 2)),
            dma((5, line, 2)),
            dma((line, chunks)),
            dma((2, line, chunks)),
            dma((2, line, chunks)),
            dma((2, line, chunks)),
            dma((2, W_CHUNKS)),
            dma((2, W_CHUNKS)),
            dma((2, line, n_t)),
            dma((2, line, n_t)),
            dma((2, line)),
            dma((2, line)),
            dma((n_t,)),
            dma((n_t,)),
            dma((n_dp,)),
            dma((n_dp,)),
        ],
        compiler_params=pltpu.CompilerParams(
            collective_id=0, has_side_effects=True, vmem_limit_bytes=63 * 2**20
        ),
    )(
        tokens_in,
        grad_out,
        gate_pre,
        up_pre,
        gate_weight,
        up_weight,
        down_weight,
        norm_gain.reshape(1, width),
    )
    return (input_grad, gain_grad.reshape(width), down_grad)


def solution(mesh):
    return jax.shard_map(
        functools.partial(per_device, mesh.shape["dp"], mesh.shape["tensor"]),
        mesh=mesh,
        in_specs=(
            P(("dp", "tensor"), None),
            P(("dp", "tensor"), None),
            P("dp", "tensor"),
            P("dp", "tensor"),
            P("dp", "tensor"),
            P("dp", "tensor"),
            P("tensor", "dp"),
            P(),
        ),
        out_specs=(P(("dp", "tensor"), None), P(), P("tensor", "dp")),
        check_vma=False,
    )
```

```python
import functools

import jax
import jax.numpy as jnp
from jax import lax
from jax.experimental import pallas as pl
from jax.experimental.pallas import tpu as pltpu
from jax.sharding import PartitionSpec as P

MESH = pl.DeviceIdType.MESH
W_CHUNKS = 4
F32 = jnp.float32
BF16 = jnp.bfloat16
NT = (((1,), (1,)), ((), ()))
TN = (((0,), (0,)), ((), ()))


def split_line(n_dp):
    assert n_dp % 4 == 0
    return n_dp // 2


def body(
    n_dp,
    n_t,
    chunks,
    tok_ref,
    out_ref,
    gate_ref,
    up_ref,
    wg_ref,
    wu_ref,
    wd_ref,
    gain_ref,
    ig_ref,
    gg_out_ref,
    dg_ref,
    x4,
    x2,
    aall,
    ysend,
    yrecv,
    own,
    zsend,
    zin,
    gp,
    ga,
    gg,
    wrecv,
    npb,
    nrv,
    gs,
    fin,
    gbuf,
    hbuf,
    s1_s,
    s1_r,
    s2_s,
    s2_r,
    ys_s,
    ys_r,
    a_s,
    a_r,
    z_s,
    z_r,
    p_s,
    p_r,
    b_s,
    b_r,
    w_s,
    w_r,
    n_s,
    n_r,
    f_s,
    f_r,
    g_s,
    g_r,
    h_s,
    h_r,
):
    r, width = tok_ref.shape
    rows, hidden = gate_ref.shape
    cols = wg_ref.shape[0]
    line = split_line(n_dp)
    rc = rows // chunks
    d = lax.axis_index("dp")
    t = lax.axis_index("tensor")
    z = d // 2
    y = d % 2
    other = 1 - y
    pair = z * 2 + other

    def loop(n, f, start=0):
        def step(i, carry):
            f(i)
            return carry

        lax.fori_loop(start, n, step, 0)

    def dp_peer(k):
        return lax.rem(d + k, n_dp)

    def t_peer(k):
        return lax.rem(t + k, n_t)

    def rcopy(src, dst, ss, rs, dd, tt):
        return pltpu.make_async_remote_copy(
            src_ref=src,
            dst_ref=dst,
            send_sem=ss,
            recv_sem=rs,
            device_id={"dp": dd, "tensor": tt},
            device_id_type=MESH,
        )

    barrier = pltpu.get_barrier_semaphore()
    loop(
        n_dp,
        lambda k: pl.semaphore_signal(
            barrier, inc=1, device_id={"dp": dp_peer(k), "tensor": t}, device_id_type=MESH
        ),
        1,
    )
    loop(
        n_t,
        lambda k: pl.semaphore_signal(
            barrier, inc=1, device_id={"dp": d, "tensor": t_peer(k)}, device_id_type=MESH
        ),
        1,
    )
    pl.semaphore_wait(barrier, n_dp + n_t - 2)

    def col(i):
        return pl.ds(pl.multiple_of(i * cols, cols), cols)

    def first(k, tgt):
        return rcopy(
            out_ref.at[:, col(tgt)], x4.at[d, t], s1_s.at[k], s1_r.at[d], tgt, t
        )

    def first_in(src):
        return rcopy(out_ref.at[:, col(0)], x4.at[src, t], s1_s.at[0], s1_r.at[src], d, t)

    loop(n_dp, lambda k: first(k, dp_peer(k)).start(), 1)

    def second(src, j):
        return rcopy(
            x4.at[src, t], x4.at[src, t], s2_s.at[src, j], s2_r.at[src, t], d, t_peer(j)
        )

    def second_in(src, tt):
        return rcopy(x4.at[src, tt], x4.at[src, tt], s2_s.at[src, 0], s2_r.at[src, tt], d, t)

    def second_own(j):
        return rcopy(
            out_ref.at[:, col(d)], x4.at[d, t], s2_s.at[d, j], s2_r.at[d, t], d, t_peer(j)
        )

    x4[d, t] = out_ref[:, col(d)]
    loop(n_t, lambda j: second_own(j).start(), 1)

    w_rows = cols // W_CHUNKS

    def weight_copy(n):
        a, c = n % 2, n // 2
        src = (wg_ref, wu_ref)[a].at[pl.ds(c * w_rows, w_rows)]
        return rcopy(
            src, wrecv.at[a, pl.ds(c * w_rows, w_rows)], w_s.at[a, c], w_r.at[a, c], pair, t
        )

    def up_copy(unit, ss, rs, way, src, side, c):
        u = unit(src, side, c)
        return rcopy(u, u, ss.at[way, src, c], rs.at[way, src, c], d + 2, t)

    def down_copy(unit, ss, rs, way, src, side, c):
        u = unit(src, side, c)
        return rcopy(u, u, ss.at[way + 1, src, c], rs.at[way + 1, src, c], d - 2, t)

    def arrived(unit, ss, rs, way, src, side, c):
        u = unit(src, side, c)
        rcopy(u, u, ss.at[way, src, c], rs.at[way, src, c], d, t).wait_recv()

    def gather_own(unit, ss, rs, way, side, c):
        @pl.when(z < line - 1)
        def _():
            up_copy(unit, ss, rs, way, z, side, c).start()

        @pl.when(z > 0)
        def _():
            down_copy(unit, ss, rs, way, z, side, c).start()

    def gather_step(unit, ss, rs, way, side, s, c, then=None):
        low, high = z - s, z + s

        @pl.when(low >= 0)
        def _():
            arrived(unit, ss, rs, way, low, side, c)

            @pl.when(z < line - 1)
            def _():
                up_copy(unit, ss, rs, way, low, side, c).start()

            if then is not None:
                then(low)

        @pl.when(high < line)
        def _():
            arrived(unit, ss, rs, way + 1, high, side, c)

            @pl.when(z > 0)
            def _():
                down_copy(unit, ss, rs, way, high, side, c).start()

            if then is not None:
                then(high)

    def gather_drain(unit, ss, rs, way, side, c):
        def one(src):
            @pl.when((src <= z) & (z < line - 1))
            def _():
                up_copy(unit, ss, rs, way, src, side, c).wait_send()

            @pl.when((src >= z) & (z > 0))
            def _():
                down_copy(unit, ss, rs, way, src, side, c).wait_send()

        loop(line, one)

    half = rows // 2
    strip = 16

    def act_unit(src, side, c):
        return aall.at[src * 2 + side, pl.ds(c * half, half)]

    def act_pair(src, c):
        u = act_unit(src, y, c)
        return rcopy(u, u, a_s.at[2, src, c], a_r.at[2, src, c], pair, t)

    def pre_unit(src, side, a):
        return gp.at[src, a]

    def pre_own(a, way):
        return rcopy(
            (gate_ref, up_ref)[a],
            gp.at[z, a],
            p_s.at[way, z, a],
            p_r.at[way, z, a],
            d + 2 - 4 * way,
            t,
        )

    for a in range(2):

        @pl.when(z < line - 1)
        def _():
            pre_own(a, 0).start()

        @pl.when(z > 0)
        def _():
            pre_own(a, 1).start()

    gp[z, 0] = gate_ref[...]
    gp[z, 1] = up_ref[...]

    def make_act(src):
        def piece(n):
            sl = pl.ds(n * strip, strip)
            gate = gp[src, 0, sl].astype(F32)
            aall[src * 2 + y, sl] = (
                gate * jax.nn.sigmoid(gate) * gp[src, 1, sl].astype(F32)
            ).astype(BF16)

        loop(rows // strip, piece)
        act_pair(src, 0).start()

    make_act(z)
    act_pair(z, 1).start()
    weight_copy(0).start()

    def relay(k):
        src = lax.rem(d + n_dp - k, n_dp)
        first_in(src).wait_recv()
        loop(n_t, lambda j: second(src, j).start(), 1)

    loop(n_dp, relay, 1)
    arrived(act_unit, a_s, a_r, 2, z, other, 1)
    gather_own(act_unit, a_s, a_r, 3, other, 1)

    def settle(src):
        loop(n_t, lambda j: second_in(src, t_peer(j)).wait_recv(), 1)
        x2[src] = x4[src].astype(F32).reshape(rows, cols).astype(BF16)

    loop(n_dp, settle)

    def cs(c):
        return pl.ds(c * rc, rc)

    def pair_part(zz, c):
        return rcopy(
            ysend.at[zz, cs(c)], yrecv.at[zz, cs(c)], ys_s.at[zz, c], ys_r.at[zz, c], pair, t
        )

    def partial(i):
        return lax.dot_general(x2[i], wd_ref[...], NT, preferred_element_type=F32)

    def send_parts(p):
        def make(q):
            zz = jnp.where(q == 0, line - 1 - p, p)
            ysend[zz] = partial(zz * 2 + other).astype(BF16)

        loop(2, make)
        for c in range(chunks):
            pair_part(line - 1 - p, c).start()
            pair_part(p, c).start()

    loop(line // 2, send_parts)

    def keep(zz):
        own[zz] = partial(zz * 2 + y)

    loop(line, keep)

    weight_copy(1).start()

    def act_step(s):
        gather_step(pre_unit, p_s, p_r, 0, y, s, 0)
        gather_step(pre_unit, p_s, p_r, 0, y, s, 1, make_act)
        gather_step(act_unit, a_s, a_r, 3, other, s, 1)

    loop(line - 1, act_step, 1)
    for n in range(2, 4):
        weight_copy(n).start()

    def line_part(way, zz, c):
        return rcopy(
            zsend.at[zz, cs(c)],
            zin.at[way, zz, cs(c)],
            z_s.at[zz, c],
            z_r.at[way, zz, c],
            d + 2 - 4 * way,
            t,
        )

    def line_in(way, zz, c):
        rcopy(
            zsend.at[zz, cs(c)], zin.at[way, zz, cs(c)], z_s.at[zz, c], z_r.at[way, zz, c], d, t
        ).wait_recv()

    def reduce_one(zz, c):
        pair_part(zz, c).wait_recv()
        own[zz, cs(c)] += yrecv[zz, cs(c)].astype(F32)

        def send_on(way, has_before):
            @pl.when(has_before)
            def _():
                line_in(way, zz, c)
                own[zz, cs(c)] += zin[way, zz, cs(c)].astype(F32)

            zsend[zz, cs(c)] = own[zz, cs(c)].astype(BF16)
            line_part(way, zz, c).start()

        @pl.when(zz > z)
        def _():
            send_on(0, z > 0)

        @pl.when(zz < z)
        def _():
            send_on(1, z < line - 1)

    def reduce_pairs(p):
        for c in range(chunks):
            reduce_one(line - 1 - p, c)
            reduce_one(p, c)

    loop(line // 2, reduce_pairs)

    def grad_unit(src, side, c):
        return ga.at[src, cs(c)]

    for c in range(chunks):

        @pl.when(z > 0)
        def _():
            line_in(0, z, c)
            own[z, cs(c)] += zin[0, z, cs(c)].astype(F32)

        @pl.when(z < line - 1)
        def _():
            line_in(1, z, c)
            own[z, cs(c)] += zin[1, z, cs(c)].astype(F32)

        ga[z, cs(c)] = own[z, cs(c)].astype(BF16)
        gather_own(grad_unit, b_s, b_r, 0, y, c)

    act_step(line - 1)
    for n in range(4, 2 * W_CHUNKS):
        weight_copy(n).start()

    def norm_copy(side, i, j):
        tt = t_peer(j)
        return rcopy(
            npb.at[side, i, tt], nrv.at[side, i, t], n_s.at[side, i, j], n_r.at[side, i, t], d, tt
        )

    def norm_own(i):
        def piece(n):
            sl = pl.ds(n * strip, strip)
            grad_act = ga[i, sl].astype(F32)
            gate = gp[i, 0, sl].astype(F32)
            sig = jax.nn.sigmoid(gate)
            gg[i, 0, sl] = (
                grad_act * gp[i, 1, sl].astype(F32) * sig * (1.0 + gate * (1.0 - sig))
            ).astype(BF16)
            gg[i, 1, sl] = (grad_act * (gate * sig)).astype(BF16)

        loop(rows // strip, piece)
        part = lax.dot_general(gg[i, 0], wg_ref[...], NT, preferred_element_type=F32)
        part = part + lax.dot_general(gg[i, 1], wu_ref[...], NT, preferred_element_type=F32)
        npb[y, i] = part.reshape(n_t, r, cols).astype(BF16)
        loop(n_t, lambda j: norm_copy(y, i, j).start(), 1)

    def norm_other(p):
        two = pl.ds(2 * p, 2)
        part = lax.dot_general(
            gg[two, 0].reshape(2 * rows, hidden), wrecv[0], NT, preferred_element_type=F32
        )
        part = part + lax.dot_general(
            gg[two, 1].reshape(2 * rows, hidden), wrecv[1], NT, preferred_element_type=F32
        )
        npb[other, two] = part.reshape(2, n_t, r, cols).astype(BF16)
        loop(2, lambda q: loop(n_t, lambda j: norm_copy(other, 2 * p + q, j).start(), 1))

    def fin_copy(side, i):
        return rcopy(
            gs.at[side, i], fin.at[z, side], f_s.at[side, i], f_r.at[side, z], i * 2 + y, t
        )

    def combine(side, i):
        def add(j, acc):
            tt = t_peer(j)
            rcopy(
                npb.at[side, i, tt], nrv.at[side, i, tt], n_s.at[side, i, 0], n_r.at[side, i, tt], d, t
            ).wait_recv()
            return acc + nrv[side, i, tt].astype(F32)

        acc = lax.fori_loop(1, n_t, add, npb[side, i, t].astype(F32)).astype(BF16)

        @pl.when(i != z)
        def _():
            gs[side, i] = acc
            fin_copy(side, i).start()

        @pl.when(i == z)
        def _():
            fin[z, side] = acc

    def at_distance(dist, f):
        def one(q):
            src = jnp.where(q == 0, z - dist, z + dist)

            @pl.when((src >= 0) & (src < line) & ((dist > 0) | (q == 0)))
            def _():
                f(src)

        loop(2, one)

    def visit(s):
        @pl.when(s > 0)
        def _():
            for c in range(chunks):
                gather_step(grad_unit, b_s, b_r, 0, y, s, c)

        at_distance(s, norm_own)

        @pl.when(s > 0)
        def _():
            at_distance(s - 1, lambda src: combine(y, src))

    loop(line, visit)
    at_distance(line - 1, lambda src: combine(y, src))

    loop(line, lambda src: arrived(act_unit, a_s, a_r, 2, src, other, 0))
    tile = 256 if hidden % 256 == 0 else hidden

    def down_tile(i):
        if tile == hidden:
            sl = slice(None)
        else:
            sl = pl.ds(pl.multiple_of(i * tile, tile), tile)
        left = aall[:, :, sl].reshape(n_dp * rows, tile)
        right = x2[...].reshape(n_dp * rows, cols)
        res = lax.dot_general(left, right, TN, preferred_element_type=F32).astype(BF16)
        if tile == hidden:
            dg_ref[...] = res
        else:
            dg_ref[sl, :] = res

    loop(hidden // tile, down_tile)

    for n in range(2 * W_CHUNKS):
        weight_copy(n).wait_recv()
    loop(line // 2, norm_other)
    loop(line, lambda i: combine(other, i))

    total = jnp.zeros((r, 1), F32)
    for i in range(n_dp):
        v = tok_ref[:, i * cols : (i + 1) * cols].astype(F32)
        total = total + jnp.sum(v * v, axis=1, keepdims=True)
    inv = lax.rsqrt(total / width + 1e-05)

    def fin_in(k):
        i = lax.rem(z + k, line)

        def one(side):
            rcopy(
                gs.at[side, i], fin.at[i, side], f_s.at[side, i], f_r.at[side, i], d, t
            ).wait_recv()

        loop(2, one)

    loop(line, fin_in, 1)

    inner = jnp.zeros((r, 1), F32)
    for i in range(n_dp):
        sl = slice(i * cols, (i + 1) * cols)
        prod = fin[i // 2, i % 2].astype(F32) * (tok_ref[:, sl].astype(F32) * inv)
        gbuf[t, :, sl] = jnp.sum(prod, axis=0, keepdims=True)
        inner = inner + jnp.sum(prod * gain_ref[:, sl], axis=1, keepdims=True)
    inner = inner / width

    def gain_copy(j):
        return rcopy(gbuf.at[t], gbuf.at[t], g_s.at[j], g_r.at[t], d, t_peer(j))

    loop(n_t, lambda j: gain_copy(j).start(), 1)
    for i in range(n_dp):
        sl = slice(i * cols, (i + 1) * cols)
        scaled = fin[i // 2, i % 2].astype(F32) * gain_ref[:, sl]
        normed = tok_ref[:, sl].astype(F32) * inv
        ig_ref[:, sl] = (
            out_ref[:, sl].astype(F32) + inv * (scaled - normed * inner)
        ).astype(BF16)

    def gain_in(j):
        tt = t_peer(j)
        rcopy(gbuf.at[tt], gbuf.at[tt], g_s.at[0], g_r.at[tt], d, t).wait_recv()

    loop(n_t, gain_in, 1)
    hbuf[d] = jnp.sum(gbuf[...], axis=0)

    def all_copy(k):
        return rcopy(hbuf.at[d], hbuf.at[d], h_s.at[k], h_r.at[d], dp_peer(k), t)

    loop(n_dp, lambda k: all_copy(k).start(), 1)

    def all_in(k):
        i = dp_peer(k)
        rcopy(hbuf.at[i], hbuf.at[i], h_s.at[0], h_r.at[i], d, t).wait_recv()

    loop(n_dp, all_in, 1)
    gg_out_ref[...] = jnp.sum(hbuf[...], axis=0)

    loop(n_dp, lambda k: first(k, dp_peer(k)).wait_send(), 1)
    loop(n_dp, lambda i: loop(n_t, lambda j: second(i, j).wait_send(), 1))
    for c in range(2):
        gather_drain(pre_unit, p_s, p_r, 0, y, c)
    gather_drain(act_unit, a_s, a_r, 3, other, 1)
    loop(line, lambda src: act_pair(src, 0).wait_send())
    act_pair(z, 1).wait_send()
    for n in range(2 * W_CHUNKS):
        weight_copy(n).wait_send()
    for c in range(chunks):
        gather_drain(grad_unit, b_s, b_r, 0, y, c)

    def drain_parts(zz):
        for c in range(chunks):
            pair_part(zz, c).wait_send()

            @pl.when(zz != z)
            def _():
                line_part(0, zz, c).wait_send()

    loop(line, drain_parts)

    def drain_norm(side):
        loop(line, lambda i: loop(n_t, lambda j: norm_copy(side, i, j).wait_send(), 1))
        loop(line, lambda k: fin_copy(side, lax.rem(z + k, line)).wait_send(), 1)

    loop(2, drain_norm)
    loop(n_t, lambda j: gain_copy(j).wait_send(), 1)
    loop(n_dp, lambda k: all_copy(k).wait_send(), 1)


def hand_on(ig_in, gain_in, dg_in, ig_out, gain_out, dg_out):
    ig_out[...] = ig_in[...]
    gain_out[...] = gain_in[...].reshape(gain_out.shape)
    dg_out[...] = dg_in[...]


def per_device(
    n_dp, n_t, tokens_in, grad_out, gate_pre, up_pre, gate_weight, up_weight, down_weight, norm_gain
):
    r, width = tokens_in.shape
    rows, hidden = gate_pre.shape
    cols = gate_weight.shape[0]
    line = split_line(n_dp)
    chunks = 4 if rows % 64 == 0 else 1
    dma = pltpu.SemaphoreType.DMA
    vmem = pl.BlockSpec(memory_space=pltpu.VMEM)
    input_grad, gain_grad, down_grad = pl.pallas_call(
        functools.partial(body, n_dp, n_t, chunks),
        out_shape=(
            jax.ShapeDtypeStruct((r, width), BF16),
            jax.ShapeDtypeStruct((1, width), F32),
            jax.ShapeDtypeStruct((hidden, cols), BF16),
        ),
        in_specs=[vmem] * 8,
        out_specs=(vmem, vmem, vmem),
        scratch_shapes=[
            pltpu.VMEM((n_dp, n_t, r, cols), BF16),
            pltpu.VMEM((n_dp, rows, cols), BF16),
            pltpu.VMEM((n_dp, rows, hidden), BF16),
            pltpu.VMEM((line, rows, hidden), BF16),
            pltpu.VMEM((line, rows, hidden), BF16),
            pltpu.VMEM((line, rows, hidden), F32),
            pltpu.VMEM((line, rows, hidden), BF16),
            pltpu.VMEM((2, line, rows, hidden), BF16),
            pltpu.VMEM((line, 2, rows, hidden), BF16),
            pltpu.VMEM((line, rows, hidden), BF16),
            pltpu.VMEM((line, 2, rows, hidden), BF16),
            pltpu.VMEM((2, cols, hidden), BF16),
            pltpu.VMEM((2, line, n_t, r, cols), BF16),
            pltpu.VMEM((2, line, n_t, r, cols), BF16),
            pltpu.VMEM((2, line, r, cols), BF16),
            pltpu.VMEM((line, 2, r, cols), BF16),
            pltpu.VMEM((n_t, 1, width), F32),
            pltpu.VMEM((n_dp, 1, width), F32),
            dma((n_dp,)),
            dma((n_dp,)),
            dma((n_dp, n_t)),
            dma((n_dp, n_t)),
            dma((line, chunks)),
            dma((line, chunks)),
            dma((5, line, 2)),
            dma((5, line, 2)),
            dma((line, chunks)),
            dma((2, line, chunks)),
            dma((2, line, 2)),
            dma((2, line, 2)),
            dma((2, line, chunks)),
            dma((2, line, chunks)),
            dma((2, W_CHUNKS)),
            dma((2, W_CHUNKS)),
            dma((2, line, n_t)),
            dma((2, line, n_t)),
            dma((2, line)),
            dma((2, line)),
            dma((n_t,)),
            dma((n_t,)),
            dma((n_dp,)),
            dma((n_dp,)),
        ],
        compiler_params=pltpu.CompilerParams(
            collective_id=0, has_side_effects=True, vmem_limit_bytes=63 * 2**20
        ),
    )(
        tokens_in,
        grad_out,
        gate_pre,
        up_pre,
        gate_weight,
        up_weight,
        down_weight,
        norm_gain.reshape(1, width),
    )
    return pl.pallas_call(
        hand_on,
        out_shape=(
            jax.ShapeDtypeStruct((r, width), BF16),
            jax.ShapeDtypeStruct((width,), F32),
            jax.ShapeDtypeStruct((hidden, cols), BF16),
        ),
        in_specs=[vmem] * 3,
        out_specs=(vmem, vmem, vmem),
    )(input_grad, gain_grad, down_grad)


def solution(mesh):
    return jax.shard_map(
        functools.partial(per_device, mesh.shape["dp"], mesh.shape["tensor"]),
        mesh=mesh,
        in_specs=(
            P(("dp", "tensor"), None),
            P(("dp", "tensor"), None),
            P("dp", "tensor"),
            P("dp", "tensor"),
            P("dp", "tensor"),
            P("dp", "tensor"),
            P("tensor", "dp"),
            P(),
        ),
        out_specs=(P(("dp", "tensor"), None), P(), P("tensor", "dp")),
        check_vma=False,
    )
```

```python
import functools

import jax
import jax.numpy as jnp
from jax import lax
from jax.experimental import pallas as pl
from jax.experimental.pallas import tpu as pltpu
from jax.sharding import PartitionSpec as P

MESH = pl.DeviceIdType.MESH
W_CHUNKS = 4
F32 = jnp.float32
BF16 = jnp.bfloat16
NT = (((1,), (1,)), ((), ()))
TN = (((0,), (0,)), ((), ()))


def split_line(n_dp):
    assert n_dp % 4 == 0
    return n_dp // 2


def body(
    n_dp,
    n_t,
    chunks,
    tok_ref,
    out_ref,
    gate_ref,
    up_ref,
    wg_ref,
    wu_ref,
    wd_ref,
    gain_ref,
    ig_ref,
    gg_out_ref,
    dg_ref,
    x4,
    x2,
    aall,
    ysend,
    yrecv,
    own,
    zsend,
    zin,
    gp,
    ga,
    gg,
    wrecv,
    npb,
    nrv,
    gs,
    fin,
    gbuf,
    hbuf,
    s1_s,
    s1_r,
    s2_s,
    s2_r,
    ys_s,
    ys_r,
    a_s,
    a_r,
    z_s,
    z_r,
    p_s,
    p_r,
    b_s,
    b_r,
    w_s,
    w_r,
    n_s,
    n_r,
    f_s,
    f_r,
    g_s,
    g_r,
    h_s,
    h_r,
):
    r, width = tok_ref.shape
    rows, hidden = gate_ref.shape
    cols = wg_ref.shape[0]
    line = split_line(n_dp)
    rc = rows // chunks
    d = lax.axis_index("dp")
    t = lax.axis_index("tensor")
    z = d // 2
    y = d % 2
    other = 1 - y
    pair = z * 2 + other

    def loop(n, f, start=0):
        def step(i, carry):
            f(i)
            return carry

        lax.fori_loop(start, n, step, 0)

    def dp_peer(k):
        return lax.rem(d + k, n_dp)

    def t_peer(k):
        return lax.rem(t + k, n_t)

    def rcopy(src, dst, ss, rs, dd, tt):
        return pltpu.make_async_remote_copy(
            src_ref=src,
            dst_ref=dst,
            send_sem=ss,
            recv_sem=rs,
            device_id={"dp": dd, "tensor": tt},
            device_id_type=MESH,
        )

    barrier = pltpu.get_barrier_semaphore()
    loop(
        n_dp,
        lambda k: pl.semaphore_signal(
            barrier, inc=1, device_id={"dp": dp_peer(k), "tensor": t}, device_id_type=MESH
        ),
        1,
    )
    loop(
        n_t,
        lambda k: pl.semaphore_signal(
            barrier, inc=1, device_id={"dp": d, "tensor": t_peer(k)}, device_id_type=MESH
        ),
        1,
    )
    pl.semaphore_wait(barrier, n_dp + n_t - 2)

    def col(i):
        return pl.ds(pl.multiple_of(i * cols, cols), cols)

    def first(k, tgt):
        return rcopy(
            out_ref.at[:, col(tgt)], x4.at[d, t], s1_s.at[k], s1_r.at[d], tgt, t
        )

    def first_in(src):
        return rcopy(out_ref.at[:, col(0)], x4.at[src, t], s1_s.at[0], s1_r.at[src], d, t)

    loop(n_dp, lambda k: first(k, dp_peer(k)).start(), 1)

    def second(src, j):
        return rcopy(
            x4.at[src, t], x4.at[src, t], s2_s.at[src, j], s2_r.at[src, t], d, t_peer(j)
        )

    def second_in(src, tt):
        return rcopy(x4.at[src, tt], x4.at[src, tt], s2_s.at[src, 0], s2_r.at[src, tt], d, t)

    def second_own(j):
        return rcopy(
            out_ref.at[:, col(d)], x4.at[d, t], s2_s.at[d, j], s2_r.at[d, t], d, t_peer(j)
        )

    x4[d, t] = out_ref[:, col(d)]
    loop(n_t, lambda j: second_own(j).start(), 1)

    w_rows = cols // W_CHUNKS

    def weight_copy(n):
        a, c = n % 2, n // 2
        src = (wg_ref, wu_ref)[a].at[pl.ds(c * w_rows, w_rows)]
        return rcopy(
            src, wrecv.at[a, pl.ds(c * w_rows, w_rows)], w_s.at[a, c], w_r.at[a, c], pair, t
        )

    def up_copy(unit, ss, rs, way, src, side, c):
        u = unit(src, side, c)
        return rcopy(u, u, ss.at[way, src, c], rs.at[way, src, c], d + 2, t)

    def down_copy(unit, ss, rs, way, src, side, c):
        u = unit(src, side, c)
        return rcopy(u, u, ss.at[way + 1, src, c], rs.at[way + 1, src, c], d - 2, t)

    def arrived(unit, ss, rs, way, src, side, c):
        u = unit(src, side, c)
        rcopy(u, u, ss.at[way, src, c], rs.at[way, src, c], d, t).wait_recv()

    def gather_own(unit, ss, rs, way, side, c):
        @pl.when(z < line - 1)
        def _():
            up_copy(unit, ss, rs, way, z, side, c).start()

        @pl.when(z > 0)
        def _():
            down_copy(unit, ss, rs, way, z, side, c).start()

    def gather_step(unit, ss, rs, way, side, s, c, then=None):
        low, high = z - s, z + s

        @pl.when(low >= 0)
        def _():
            arrived(unit, ss, rs, way, low, side, c)

            @pl.when(z < line - 1)
            def _():
                up_copy(unit, ss, rs, way, low, side, c).start()

            if then is not None:
                then(low)

        @pl.when(high < line)
        def _():
            arrived(unit, ss, rs, way + 1, high, side, c)

            @pl.when(z > 0)
            def _():
                down_copy(unit, ss, rs, way, high, side, c).start()

            if then is not None:
                then(high)

    def gather_drain(unit, ss, rs, way, side, c):
        def one(src):
            @pl.when((src <= z) & (z < line - 1))
            def _():
                up_copy(unit, ss, rs, way, src, side, c).wait_send()

            @pl.when((src >= z) & (z > 0))
            def _():
                down_copy(unit, ss, rs, way, src, side, c).wait_send()

        loop(line, one)

    far = rows * 3 // 4
    strip = 16

    def act_unit(src, side, c):
        at = (0, rows - far)[c]
        return aall.at[src * 2 + side, pl.ds(at, (rows - far, far)[c])]

    def act_pair(src, c):
        u = act_unit(src, y, c)
        return rcopy(u, u, a_s.at[2, src, c], a_r.at[2, src, c], pair, t)

    def pre_unit(src, side, a):
        return gp.at[src, a]

    def pre_own(a, way):
        return rcopy(
            (gate_ref, up_ref)[a],
            gp.at[z, a],
            p_s.at[way, z, a],
            p_r.at[way, z, a],
            d + 2 - 4 * way,
            t,
        )

    for a in range(2):

        @pl.when(z < line - 1)
        def _():
            pre_own(a, 0).start()

        @pl.when(z > 0)
        def _():
            pre_own(a, 1).start()

    gp[z, 0] = gate_ref[...]
    gp[z, 1] = up_ref[...]

    def make_act(src):
        def piece(n):
            sl = pl.ds(n * strip, strip)
            gate = gp[src, 0, sl].astype(F32)
            aall[src * 2 + y, sl] = (
                gate * jax.nn.sigmoid(gate) * gp[src, 1, sl].astype(F32)
            ).astype(BF16)

        loop(rows // strip, piece)
        act_pair(src, 0).start()

    make_act(z)
    act_pair(z, 1).start()
    weight_copy(0).start()

    def relay(k):
        src = lax.rem(d + n_dp - k, n_dp)
        first_in(src).wait_recv()
        loop(n_t, lambda j: second(src, j).start(), 1)

    loop(n_dp, relay, 1)
    arrived(act_unit, a_s, a_r, 2, z, other, 1)
    gather_own(act_unit, a_s, a_r, 3, other, 1)

    def settle(src):
        loop(n_t, lambda j: second_in(src, t_peer(j)).wait_recv(), 1)
        x2[src] = x4[src].astype(F32).reshape(rows, cols).astype(BF16)

    loop(n_dp, settle)

    def cs(c):
        return pl.ds(c * rc, rc)

    def pair_part(zz, c):
        return rcopy(
            ysend.at[zz, cs(c)], yrecv.at[zz, cs(c)], ys_s.at[zz, c], ys_r.at[zz, c], pair, t
        )

    def partial(i):
        return lax.dot_general(x2[i], wd_ref[...], NT, preferred_element_type=F32)

    def send_parts(p):
        def make(q):
            zz = jnp.where(q == 0, line - 1 - p, p)
            ysend[zz] = partial(zz * 2 + other).astype(BF16)

        loop(2, make)
        for c in range(chunks):
            pair_part(line - 1 - p, c).start()
            pair_part(p, c).start()

    loop(line // 2, send_parts)

    def keep(zz):
        own[zz] = partial(zz * 2 + y)

    loop(line, keep)

    weight_copy(1).start()

    def act_step(s):
        gather_step(pre_unit, p_s, p_r, 0, y, s, 0)
        gather_step(pre_unit, p_s, p_r, 0, y, s, 1, make_act)
        gather_step(act_unit, a_s, a_r, 3, other, s, 1)

    loop(line - 1, act_step, 1)
    for n in range(2, 4):
        weight_copy(n).start()

    def line_part(way, zz, c):
        return rcopy(
            zsend.at[zz, cs(c)],
            zin.at[way, zz, cs(c)],
            z_s.at[zz, c],
            z_r.at[way, zz, c],
            d + 2 - 4 * way,
            t,
        )

    def line_in(way, zz, c):
        rcopy(
            zsend.at[zz, cs(c)], zin.at[way, zz, cs(c)], z_s.at[zz, c], z_r.at[way, zz, c], d, t
        ).wait_recv()

    def reduce_one(zz, c):
        pair_part(zz, c).wait_recv()
        own[zz, cs(c)] += yrecv[zz, cs(c)].astype(F32)

        def send_on(way, has_before):
            @pl.when(has_before)
            def _():
                line_in(way, zz, c)
                own[zz, cs(c)] += zin[way, zz, cs(c)].astype(F32)

            zsend[zz, cs(c)] = own[zz, cs(c)].astype(BF16)
            line_part(way, zz, c).start()

        @pl.when(zz > z)
        def _():
            send_on(0, z > 0)

        @pl.when(zz < z)
        def _():
            send_on(1, z < line - 1)

    def reduce_pairs(p):
        for c in range(chunks):
            reduce_one(line - 1 - p, c)
            reduce_one(p, c)

    loop(line // 2, reduce_pairs)

    def grad_unit(src, side, c):
        return ga.at[src, cs(c)]

    for c in range(chunks):

        @pl.when(z > 0)
        def _():
            line_in(0, z, c)
            own[z, cs(c)] += zin[0, z, cs(c)].astype(F32)

        @pl.when(z < line - 1)
        def _():
            line_in(1, z, c)
            own[z, cs(c)] += zin[1, z, cs(c)].astype(F32)

        ga[z, cs(c)] = own[z, cs(c)].astype(BF16)
        gather_own(grad_unit, b_s, b_r, 0, y, c)

    act_step(line - 1)
    for n in range(4, 2 * W_CHUNKS):
        weight_copy(n).start()

    def norm_copy(side, i, j):
        tt = t_peer(j)
        return rcopy(
            npb.at[side, i, tt], nrv.at[side, i, t], n_s.at[side, i, j], n_r.at[side, i, t], d, tt
        )

    def norm_own(i):
        def piece(n):
            sl = pl.ds(n * strip, strip)
            grad_act = ga[i, sl].astype(F32)
            gate = gp[i, 0, sl].astype(F32)
            sig = jax.nn.sigmoid(gate)
            gg[i, 0, sl] = (
                grad_act * gp[i, 1, sl].astype(F32) * sig * (1.0 + gate * (1.0 - sig))
            ).astype(BF16)
            gg[i, 1, sl] = (grad_act * (gate * sig)).astype(BF16)

        loop(rows // strip, piece)
        part = lax.dot_general(gg[i, 0], wg_ref[...], NT, preferred_element_type=F32)
        part = part + lax.dot_general(gg[i, 1], wu_ref[...], NT, preferred_element_type=F32)
        npb[y, i] = part.reshape(n_t, r, cols).astype(BF16)
        loop(n_t, lambda j: norm_copy(y, i, j).start(), 1)

    def norm_other(p):
        two = pl.ds(2 * p, 2)
        part = lax.dot_general(
            gg[two, 0].reshape(2 * rows, hidden), wrecv[0], NT, preferred_element_type=F32
        )
        part = part + lax.dot_general(
            gg[two, 1].reshape(2 * rows, hidden), wrecv[1], NT, preferred_element_type=F32
        )
        npb[other, two] = part.reshape(2, n_t, r, cols).astype(BF16)
        loop(2, lambda q: loop(n_t, lambda j: norm_copy(other, 2 * p + q, j).start(), 1))

    def fin_copy(side, i):
        return rcopy(
            gs.at[side, i], fin.at[z, side], f_s.at[side, i], f_r.at[side, z], i * 2 + y, t
        )

    def combine(side, i):
        def add(j, acc):
            tt = t_peer(j)
            rcopy(
                npb.at[side, i, tt], nrv.at[side, i, tt], n_s.at[side, i, 0], n_r.at[side, i, tt], d, t
            ).wait_recv()
            return acc + nrv[side, i, tt].astype(F32)

        acc = lax.fori_loop(1, n_t, add, npb[side, i, t].astype(F32)).astype(BF16)

        @pl.when(i != z)
        def _():
            gs[side, i] = acc
            fin_copy(side, i).start()

        @pl.when(i == z)
        def _():
            fin[z, side] = acc

    def at_distance(dist, f):
        def one(q):
            src = jnp.where(q == 0, z - dist, z + dist)

            @pl.when((src >= 0) & (src < line) & ((dist > 0) | (q == 0)))
            def _():
                f(src)

        loop(2, one)

    def visit(s):
        @pl.when(s > 0)
        def _():
            for c in range(chunks):
                gather_step(grad_unit, b_s, b_r, 0, y, s, c)

        at_distance(s, norm_own)

        @pl.when(s > 0)
        def _():
            at_distance(s - 1, lambda src: combine(y, src))

    loop(line, visit)
    at_distance(line - 1, lambda src: combine(y, src))

    loop(line, lambda src: arrived(act_unit, a_s, a_r, 2, src, other, 0))
    tile = 256 if hidden % 256 == 0 else hidden

    def down_tile(i):
        if tile == hidden:
            sl = slice(None)
        else:
            sl = pl.ds(pl.multiple_of(i * tile, tile), tile)
        left = aall[:, :, sl].reshape(n_dp * rows, tile)
        right = x2[...].reshape(n_dp * rows, cols)
        res = lax.dot_general(left, right, TN, preferred_element_type=F32).astype(BF16)
        if tile == hidden:
            dg_ref[...] = res
        else:
            dg_ref[sl, :] = res

    loop(hidden // tile, down_tile)

    for n in range(2 * W_CHUNKS):
        weight_copy(n).wait_recv()
    loop(line // 2, norm_other)
    loop(line, lambda i: combine(other, i))

    total = jnp.zeros((r, 1), F32)
    for i in range(n_dp):
        v = tok_ref[:, i * cols : (i + 1) * cols].astype(F32)
        total = total + jnp.sum(v * v, axis=1, keepdims=True)
    inv = lax.rsqrt(total / width + 1e-05)

    def fin_in(k):
        i = lax.rem(z + k, line)

        def one(side):
            rcopy(
                gs.at[side, i], fin.at[i, side], f_s.at[side, i], f_r.at[side, i], d, t
            ).wait_recv()

        loop(2, one)

    loop(line, fin_in, 1)

    inner = jnp.zeros((r, 1), F32)
    for i in range(n_dp):
        sl = slice(i * cols, (i + 1) * cols)
        prod = fin[i // 2, i % 2].astype(F32) * (tok_ref[:, sl].astype(F32) * inv)
        gbuf[t, :, sl] = jnp.sum(prod, axis=0, keepdims=True)
        inner = inner + jnp.sum(prod * gain_ref[:, sl], axis=1, keepdims=True)
    inner = inner / width

    def gain_copy(j):
        return rcopy(gbuf.at[t], gbuf.at[t], g_s.at[j], g_r.at[t], d, t_peer(j))

    loop(n_t, lambda j: gain_copy(j).start(), 1)
    for i in range(n_dp):
        sl = slice(i * cols, (i + 1) * cols)
        scaled = fin[i // 2, i % 2].astype(F32) * gain_ref[:, sl]
        normed = tok_ref[:, sl].astype(F32) * inv
        ig_ref[:, sl] = (
            out_ref[:, sl].astype(F32) + inv * (scaled - normed * inner)
        ).astype(BF16)

    def gain_in(j):
        tt = t_peer(j)
        rcopy(gbuf.at[tt], gbuf.at[tt], g_s.at[0], g_r.at[tt], d, t).wait_recv()

    loop(n_t, gain_in, 1)
    hbuf[d] = jnp.sum(gbuf[...], axis=0)

    def all_copy(k):
        return rcopy(hbuf.at[d], hbuf.at[d], h_s.at[k], h_r.at[d], dp_peer(k), t)

    loop(n_dp, lambda k: all_copy(k).start(), 1)

    def all_in(k):
        i = dp_peer(k)
        rcopy(hbuf.at[i], hbuf.at[i], h_s.at[0], h_r.at[i], d, t).wait_recv()

    loop(n_dp, all_in, 1)
    gg_out_ref[...] = jnp.sum(hbuf[...], axis=0)

    loop(n_dp, lambda k: first(k, dp_peer(k)).wait_send(), 1)
    loop(n_dp, lambda i: loop(n_t, lambda j: second(i, j).wait_send(), 1))
    for c in range(2):
        gather_drain(pre_unit, p_s, p_r, 0, y, c)
    gather_drain(act_unit, a_s, a_r, 3, other, 1)
    loop(line, lambda src: act_pair(src, 0).wait_send())
    act_pair(z, 1).wait_send()
    for n in range(2 * W_CHUNKS):
        weight_copy(n).wait_send()
    for c in range(chunks):
        gather_drain(grad_unit, b_s, b_r, 0, y, c)

    def drain_parts(zz):
        for c in range(chunks):
            pair_part(zz, c).wait_send()

            @pl.when(zz != z)
            def _():
                line_part(0, zz, c).wait_send()

    loop(line, drain_parts)

    def drain_norm(side):
        loop(line, lambda i: loop(n_t, lambda j: norm_copy(side, i, j).wait_send(), 1))
        loop(line, lambda k: fin_copy(side, lax.rem(z + k, line)).wait_send(), 1)

    loop(2, drain_norm)
    loop(n_t, lambda j: gain_copy(j).wait_send(), 1)
    loop(n_dp, lambda k: all_copy(k).wait_send(), 1)


def hand_on(ig_in, gain_in, dg_in, ig_out, gain_out, dg_out):
    ig_out[...] = ig_in[...]
    gain_out[...] = gain_in[...].reshape(gain_out.shape)
    dg_out[...] = dg_in[...]


def per_device(
    n_dp, n_t, tokens_in, grad_out, gate_pre, up_pre, gate_weight, up_weight, down_weight, norm_gain
):
    r, width = tokens_in.shape
    rows, hidden = gate_pre.shape
    cols = gate_weight.shape[0]
    line = split_line(n_dp)
    chunks = 4 if rows % 64 == 0 else 1
    dma = pltpu.SemaphoreType.DMA
    vmem = pl.BlockSpec(memory_space=pltpu.VMEM)
    input_grad, gain_grad, down_grad = pl.pallas_call(
        functools.partial(body, n_dp, n_t, chunks),
        out_shape=(
            jax.ShapeDtypeStruct((r, width), BF16),
            jax.ShapeDtypeStruct((1, width), F32),
            jax.ShapeDtypeStruct((hidden, cols), BF16),
        ),
        in_specs=[vmem] * 8,
        out_specs=(vmem, vmem, vmem),
        scratch_shapes=[
            pltpu.VMEM((n_dp, n_t, r, cols), BF16),
            pltpu.VMEM((n_dp, rows, cols), BF16),
            pltpu.VMEM((n_dp, rows, hidden), BF16),
            pltpu.VMEM((line, rows, hidden), BF16),
            pltpu.VMEM((line, rows, hidden), BF16),
            pltpu.VMEM((line, rows, hidden), F32),
            pltpu.VMEM((line, rows, hidden), BF16),
            pltpu.VMEM((2, line, rows, hidden), BF16),
            pltpu.VMEM((line, 2, rows, hidden), BF16),
            pltpu.VMEM((line, rows, hidden), BF16),
            pltpu.VMEM((line, 2, rows, hidden), BF16),
            pltpu.VMEM((2, cols, hidden), BF16),
            pltpu.VMEM((2, line, n_t, r, cols), BF16),
            pltpu.VMEM((2, line, n_t, r, cols), BF16),
            pltpu.VMEM((2, line, r, cols), BF16),
            pltpu.VMEM((line, 2, r, cols), BF16),
            pltpu.VMEM((n_t, 1, width), F32),
            pltpu.VMEM((n_dp, 1, width), F32),
            dma((n_dp,)),
            dma((n_dp,)),
            dma((n_dp, n_t)),
            dma((n_dp, n_t)),
            dma((line, chunks)),
            dma((line, chunks)),
            dma((5, line, 2)),
            dma((5, line, 2)),
            dma((line, chunks)),
            dma((2, line, chunks)),
            dma((2, line, 2)),
            dma((2, line, 2)),
            dma((2, line, chunks)),
            dma((2, line, chunks)),
            dma((2, W_CHUNKS)),
            dma((2, W_CHUNKS)),
            dma((2, line, n_t)),
            dma((2, line, n_t)),
            dma((2, line)),
            dma((2, line)),
            dma((n_t,)),
            dma((n_t,)),
            dma((n_dp,)),
            dma((n_dp,)),
        ],
        compiler_params=pltpu.CompilerParams(
            collective_id=0, has_side_effects=True, vmem_limit_bytes=63 * 2**20
        ),
    )(
        tokens_in,
        grad_out,
        gate_pre,
        up_pre,
        gate_weight,
        up_weight,
        down_weight,
        norm_gain.reshape(1, width),
    )
    return pl.pallas_call(
        hand_on,
        out_shape=(
            jax.ShapeDtypeStruct((r, width), BF16),
            jax.ShapeDtypeStruct((width,), F32),
            jax.ShapeDtypeStruct((hidden, cols), BF16),
        ),
        in_specs=[vmem] * 3,
        out_specs=(vmem, vmem, vmem),
    )(input_grad, gain_grad, down_grad)


def solution(mesh):
    return jax.shard_map(
        functools.partial(per_device, mesh.shape["dp"], mesh.shape["tensor"]),
        mesh=mesh,
        in_specs=(
            P(("dp", "tensor"), None),
            P(("dp", "tensor"), None),
            P("dp", "tensor"),
            P("dp", "tensor"),
            P("dp", "tensor"),
            P("dp", "tensor"),
            P("tensor", "dp"),
            P(),
        ),
        out_specs=(P(("dp", "tensor"), None), P(), P("tensor", "dp")),
        check_vma=False,
    )
```
